32 devices in a mesh: groups: 2 (over x), chol: 16 (over z, y, core).
Axes of the slice: x: 2, y: 2, z: 4, core: 2. Of those that a mesh axis runs over, the one named last changes fastest.
Arguments:
- green_rows: bfloat16 [128, 65536], P('groups', 'chol'), parts along dimension 0, may hold values from -6 to 6
- factors: bfloat16 [5120, 65536], P(None, 'chol'), may hold values from -0.03125 to 0.03125
- noise_draws: float32 [128, 5120], P('groups', 'chol'), parts along dimension 0, may hold values from -6 to 6
Outputs:
- potential: float32 [128, 65536], P('groups', 'chol'), parts along dimension 0
- log_weight: float32 [128], P(('groups', 'chol')), parts along dimension 0
The draws below stay inside these ranges and needn't reach their ends.
There are 2 independent parts, one for each index of `groups`. The reference program is written for one: setup_inputs(seed, part) draws one part's arguments, and reference() takes and returns one part's arrays. A program takes and returns all parts, laid end to end along the dimension named above; an argument that names none is the same for every part. Nothing has to cross between parts.
All inputs are finite; a program needn't handle non-finite values.
Results may differ from the reference program's by a relative error of at most 0.0029.
Values may be sent and summed in bfloat16 or wider, within the bound.
A program may use at most 128 MiB of HBM per device.

```python
import math
import jax
import jax.numpy as jnp
from jax import lax

NCHOL = 5120
PAIRS = 65536
WALKERS = 64


def strengthened(array, stream_key, source, target, blocks, factor):
    def block_of(position):
        return (jnp.arange(array.shape[position]) // (array.shape[position] // blocks)).reshape((-1,) + (1,) * (array.ndim - 1 - position))

    one_side = jax.random.permutation(stream_key, blocks)[block_of(target)]
    other_side = (block_of(target) + blocks // 2) % blocks
    return jnp.where((block_of(source) == one_side) | (block_of(source) == other_side), factor * array, array)


def block_scale(key, dims, cuts, smallest, top_value):
    def one(dim, shards_of):
        steps = jax.random.uniform(jax.random.fold_in(jax.random.fold_in(key, 6), dim), (shards_of,), jnp.float32, smallest / len(cuts), top_value / len(cuts))
        return jnp.repeat(jnp.exp(steps), dims[dim] // shards_of).reshape((-1,) + (1,) * (len(dims) - dim - 1))

    loudness = one(*cuts[0])
    for cut in cuts[1:]:
        loudness = loudness * one(*cut)
    return loudness


def gaussian(own_key, dims, scale, most, cuts=(), dtype=jnp.bfloat16):
    entries = scale * jax.random.normal(own_key, dims, jnp.float32)
    if cuts:
        entries = entries * block_scale(own_key, dims, cuts, -0.22, 0.18)
    return jnp.clip(entries, -most, most).astype(dtype)


def noise_with(own_key, shape, spread, bound, pieces, heavy, held_as=jnp.bfloat16):
    result = spread * jax.random.normal(own_key, shape, jnp.float32)
    if pieces:
        result = result * block_scale(own_key, shape, pieces, -0.22, 0.18)
    return jnp.clip(strengthened(result, jax.random.fold_in(own_key, 3), *heavy), -bound, bound).astype(held_as)


def setup_inputs(seed: int = 0, part: int = 0) -> dict:
    key_list = jax.random.split(jax.random.key(seed), 4)
    part_keys = jax.random.split(jax.random.fold_in(key_list[3], part), 4)
    return {
        "green_rows": gaussian(part_keys[0], (WALKERS, PAIRS), 1.0, 6.0, ((1, 16),)),
        "factors": noise_with(key_list[1], (NCHOL, PAIRS), PAIRS ** -0.5, 0.03125, ((1, 16),), (1, 0, 16, 2.0)),
        "noise_draws": gaussian(part_keys[2], (WALKERS, NCHOL), 1.0, 6.0, ((1, 16),), jnp.float32),
    }


def reference(green_rows, factors, noise_draws):
    forces = lax.dot_general(green_rows, factors, (((1,), (1,)), ((), ())), preferred_element_type=jnp.float32)
    capped = jnp.tanh(forces)
    fields = noise_draws - capped
    potential = jnp.dot(fields.astype(jnp.bfloat16), factors, preferred_element_type=jnp.float32)
    log_weight = lax.optimization_barrier(jnp.sum(fields * capped - 0.5 * capped * capped, axis=1)) / math.sqrt(NCHOL)
    return (potential, log_weight)
```

```python
import functools
import math

import jax
import jax.numpy as jnp
from jax import lax
from jax.experimental import pallas as pl
from jax.experimental.pallas import tpu as pltpu
from jax.sharding import PartitionSpec as P

MESH = pl.DeviceIdType.MESH
STAGES = 4


def flip(a, b, bits):
    total = 0
    for bit in range(bits):
        x = lax.rem(lax.div(a, 2**bit), 2)
        y = lax.rem(lax.div(b, 2**bit), 2) if not isinstance(b, int) else (b >> bit) & 1
        total = total + (x + y - 2 * x * y) * 2**bit
    return total


def kernel(n, pack, green, factors, noise, pot, logw, fac, own, d2d_out, d2d_in, rs_in, ag, nz,
           lhs, lw, lws, fac_sem, ds, dr, rs, rr, gs, gr, fs, fr, ls, lr, ps, pr):
    chips = n // 2
    bits = chips.bit_length() - 1
    total = factors.shape[0]
    nv = total // n
    half = nv // pack
    walkers = green.shape[0]
    me = lax.axis_index("chol")
    chip, core = lax.div(me, 2), lax.rem(me, 2)
    other = 1 - core
    partner = chip * 2 + other

    def peer(k):
        return flip(chip, k, bits) * 2 + core

    def load(i):
        k = chips - 1 - i
        rows = pl.ds(pl.multiple_of(flip(chip, k, bits) * (2 * nv), 2 * nv), 2 * nv)
        return pltpu.make_async_copy(factors.at[rows, :], fac.at[rows, :], fac_sem.at[k])

    def start_load(i, c):
        load(i).start()
        return c

    lax.fori_loop(0, chips, start_load, 0)

    barrier = pltpu.get_barrier_semaphore()
    pl.semaphore_signal(barrier, inc=1, device_id={"chol": partner}, device_id_type=MESH)

    def greet(k, c):
        pl.semaphore_signal(barrier, inc=1, device_id={"chol": peer(k)}, device_id_type=MESH)
        return c

    lax.fori_loop(1, chips, greet, 0)
    turned = noise[...].T
    nz[...] = jnp.concatenate([turned[j * half:(j + 1) * half] for j in range(pack)], axis=1)
    pl.semaphore_wait(barrier, chips)

    def remote(src, dst, s, r, to):
        return pltpu.make_async_remote_copy(
            src_ref=src, dst_ref=dst, send_sem=s, recv_sem=r,
            device_id={"chol": to}, device_id_type=MESH)

    def d2d(k):
        return remote(d2d_out.at[k], d2d_in.at[k], ds.at[k], dr.at[k], partner)

    def scatter(k):
        return remote(own.at[k], rs_in.at[k], rs.at[k], rr.at[k], peer(k))

    def partial(k, which):
        base = (flip(chip, k, bits) * 2 + which) * nv
        parts = []
        for j in range(pack):
            rows = pl.ds(pl.multiple_of(base + j * half, 16), half)
            parts.append(lax.dot_general(fac[rows, :], green[...], (((1,), (1,)), ((), ())),
                                         preferred_element_type=jnp.float32))
        return jnp.concatenate(parts, axis=1) if pack > 1 else parts[0]

    def finish(k):
        d2d(k).wait_recv()
        own[k] = own[k] + d2d_in[k]

    def step(i, c):
        k = chips - 1 - i
        load(i).wait()
        d2d_out[k] = partial(k, other)
        d2d(k).start()

        @pl.when(i > 0)
        def _():
            finish(k + 1)
            scatter(k + 1).start()

        own[k] = partial(k, core)
        return c

    lax.fori_loop(0, chips, step, 0)
    finish(0)

    def gather_sum(k, acc):
        scatter(k).wait_recv()
        return acc + rs_in[k]

    forces = lax.fori_loop(1, chips, gather_sum, own[0])
    capped = jnp.tanh(forces)
    fields = nz[...] - capped

    def spread(k):
        mine = ag.at[0, core]
        return remote(mine, ag.at[k, core], gs.at[k], gr.at[k], peer(k))

    def forward(k):
        return remote(ag.at[k, core], ag.at[k, core], fs.at[k], fr.at[k], partner)

    def forward_in(k):
        return remote(ag.at[k, other], ag.at[k, other], fs.at[k], fr.at[k], partner)

    def tell(k):
        return remote(lw.at[0], lw.at[k], ls.at[k], lr.at[k], peer(k))

    pair_sum = remote(lws.at[0], lws.at[1], ps, pr, partner)

    ag[0, core] = fields.astype(jnp.bfloat16)
    forward(0).start()

    def start_spread(k, c):
        spread(k).start()
        return c

    lax.fori_loop(1, chips, start_spread, 0)
    row = jnp.sum(fields * capped - 0.5 * capped * capped, axis=0, keepdims=True)
    lw[0] = jnp.broadcast_to(row, lw.shape[1:])

    def start_tell(k, c):
        tell(k).start()
        return c

    lax.fori_loop(1, chips, start_tell, 0)

    per_stage = chips // STAGES
    deep = total // STAGES
    own_stage = lax.div(chip, per_stage)
    cols = pot.shape[1]
    width = min(512, cols // 2)
    halves = cols // 2 // width

    def pull(s):
        def one(k, c):
            spread(k).wait_recv()
            forward(k).start()
            return c
        lax.fori_loop(max(1, s * per_stage), (s + 1) * per_stage, one, 0)

    def settle(s):
        def one(k, c):
            forward_in(k).wait_recv()
            return c
        lax.fori_loop(s * per_stage, (s + 1) * per_stage, one, 0)

    pull(0)
    settle(0)
    for s in range(STAGES):
        plane = flip(own_stage, s, 2)
        blocks = []
        for m in range(per_stage):
            k = flip(plane * per_stage + m, chip, bits)
            for c in range(2):
                block = ag[k, c]
                for j in range(pack):
                    blocks.append(block[:, j * walkers:(j + 1) * walkers])
        lhs[...] = jnp.concatenate(blocks, axis=0).T
        rows = pl.ds(pl.multiple_of(plane * deep, deep), deep)

        def column(t, c, s=s, rows=rows):
            at = pl.ds(pl.multiple_of(t * width, width), width)
            value = jnp.dot(lhs[...], fac[rows, at], preferred_element_type=jnp.float32)
            pot[:, at] = value if s == 0 else pot[:, at] + value
            return c

        lax.fori_loop(0, halves, column, 0)
        if s + 1 < STAGES:
            pull(s + 1)
        if s == STAGES - 2:
            def add(k, acc):
                tell(k).wait_recv()
                return acc + lw[k]
            lws[0] = lax.fori_loop(1, chips, add, lw[0])
            pair_sum.start()
        lax.fori_loop(halves, 2 * halves, column, 0)
        if s + 1 < STAGES:
            settle(s + 1)

    pair_sum.wait()
    packed = lws[0, 0:1, :] + lws[1, 0:1, :]
    row = packed[:, 0:walkers]
    for j in range(1, pack):
        row = row + packed[:, j * walkers:(j + 1) * walkers]
    per = walkers // n
    wide = jnp.broadcast_to(row, (per, walkers))
    here = lax.broadcasted_iota(jnp.int32, (per, walkers), 1) == (
        me * per + lax.broadcasted_iota(jnp.int32, (per, walkers), 0))
    logw[...] = jnp.sum(jnp.where(here, wide, 0.0), axis=1, keepdims=True) / math.sqrt(total)

    d2d(0).wait_send()
    forward(0).wait_send()

    def drain(k, c):
        d2d(k).wait_send()
        scatter(k).wait_send()
        spread(k).wait_send()
        forward(k).wait_send()
        tell(k).wait_send()
        return c

    lax.fori_loop(1, chips, drain, 0)


def solution(mesh):
    n = mesh.shape["chol"]

    def per_device(green, factors, noise):
        walkers, cols = green.shape
        total = factors.shape[0]
        chips = n // 2
        pack = max(1, 128 // walkers)
        half, lanes = total // n // pack, walkers * pack
        vmem = pl.BlockSpec(memory_space=pltpu.VMEM)
        dma = pltpu.SemaphoreType.DMA
        block = pltpu.VMEM((chips, half, lanes), jnp.float32)
        pot, logw = pl.pallas_call(
            functools.partial(kernel, n, pack),
            out_shape=(jax.ShapeDtypeStruct((walkers, cols), jnp.float32),
                       jax.ShapeDtypeStruct((walkers // n, 1), jnp.float32)),
            in_specs=[vmem, pl.BlockSpec(memory_space=pl.ANY), vmem],
            out_specs=(vmem, vmem),
            scratch_shapes=[
                pltpu.VMEM(factors.shape, jnp.bfloat16),
                block, block, block, block,
                pltpu.VMEM((chips, 2, half, lanes), jnp.bfloat16),
                pltpu.VMEM((half, lanes), jnp.float32),
                pltpu.VMEM((walkers, total // STAGES), jnp.bfloat16),
                pltpu.VMEM((chips, 8, lanes), jnp.float32),
                pltpu.VMEM((2, 8, lanes), jnp.float32),
            ] + [dma((chips,))] * 11 + [dma, dma],
            compiler_params=pltpu.CompilerParams(
                collective_id=0, has_side_effects=True, vmem_limit_bytes=67043328),
        )(green, factors, noise)
        return pot, logw.reshape(-1)

    return jax.shard_map(
        per_device,
        mesh=mesh,
        in_specs=(P("groups", "chol"), P(None, "chol"), P("groups", "chol")),
        out_specs=(P("groups", "chol"), P(("groups", "chol"))),
        check_vma=False,
    )
```

```python
import functools
import math

import jax
import jax.numpy as jnp
from jax import lax
from jax.experimental import pallas as pl
from jax.experimental.pallas import tpu as pltpu
from jax.sharding import PartitionSpec as P

MESH = pl.DeviceIdType.MESH
STAGES = 4


def flip(a, b, bits):
    total = 0
    for bit in range(bits):
        x = lax.rem(lax.div(a, 2**bit), 2)
        y = lax.rem(lax.div(b, 2**bit), 2) if not isinstance(b, int) else (b >> bit) & 1
        total = total + (x + y - 2 * x * y) * 2**bit
    return total


def kernel(n, pack, green, factors, noise, pot, logw, fac, own, d2d_out, d2d_in, rs_in, ag, nz,
           lhs, lw, lws, fac_sem, ds, dr, rs, rr, gs, gr, fs, fr, ls, lr, ps, pr):
    chips = n // 2
    bits = chips.bit_length() - 1
    total = factors.shape[0]
    nv = total // n
    half = nv // pack
    walkers = green.shape[0]
    me = lax.axis_index("chol")
    chip, core = lax.div(me, 2), lax.rem(me, 2)
    other = 1 - core
    partner = chip * 2 + other

    def peer(k):
        return flip(chip, k, bits) * 2 + core

    def load(i):
        k = chips - 1 - i
        rows = pl.ds(pl.multiple_of(flip(chip, k, bits) * (2 * nv), 2 * nv), 2 * nv)
        return pltpu.make_async_copy(factors.at[rows, :], fac.at[rows, :], fac_sem.at[k])

    def start_load(i, c):
        load(i).start()
        return c

    lax.fori_loop(0, chips, start_load, 0)

    barrier = pltpu.get_barrier_semaphore()
    pl.semaphore_signal(barrier, inc=1, device_id={"chol": partner}, device_id_type=MESH)

    def greet(k, c):
        pl.semaphore_signal(barrier, inc=1, device_id={"chol": peer(k)}, device_id_type=MESH)
        return c

    lax.fori_loop(1, chips, greet, 0)
    turned = noise[...].T
    nz[...] = jnp.concatenate([turned[j * half:(j + 1) * half] for j in range(pack)], axis=1)
    pl.semaphore_wait(barrier, chips)

    def remote(src, dst, s, r, to):
        return pltpu.make_async_remote_copy(
            src_ref=src, dst_ref=dst, send_sem=s, recv_sem=r,
            device_id={"chol": to}, device_id_type=MESH)

    def d2d(k):
        return remote(d2d_out.at[k], d2d_in.at[k], ds.at[k], dr.at[k], partner)

    def scatter(k):
        return remote(own.at[k], rs_in.at[k], rs.at[k], rr.at[k], peer(k))

    def partial(k, which):
        base = (flip(chip, k, bits) * 2 + which) * nv
        parts = []
        for j in range(pack):
            rows = pl.ds(pl.multiple_of(base + j * half, 16), half)
            parts.append(lax.dot_general(fac[rows, :], green[...], (((1,), (1,)), ((), ())),
                                         preferred_element_type=jnp.float32))
        return jnp.concatenate(parts, axis=1) if pack > 1 else parts[0]

    def finish(k):
        d2d(k).wait_recv()
        own[k] = own[k] + d2d_in[k]

    def step(i, c):
        k = chips - 1 - i
        load(i).wait()
        d2d_out[k] = partial(k, other)
        d2d(k).start()

        @pl.when(i > 0)
        def _():
            finish(k + 1)
            scatter(k + 1).start()

        own[k] = partial(k, core)
        return c

    lax.fori_loop(0, chips, step, 0)
    finish(0)

    def gather_sum(k, acc):
        scatter(k).wait_recv()
        return acc + rs_in[k]

    forces = lax.fori_loop(1, chips, gather_sum, own[0])
    capped = jnp.tanh(forces)
    fields = nz[...] - capped

    def spread(k):
        mine = ag.at[0, core]
        return remote(mine, ag.at[k, core], gs.at[k], gr.at[k], peer(k))

    def forward(k):
        return remote(ag.at[k, core], ag.at[k, core], fs.at[k], fr.at[k], partner)

    def forward_in(k):
        return remote(ag.at[k, other], ag.at[k, other], fs.at[k], fr.at[k], partner)

    def tell(k):
        return remote(lw.at[0], lw.at[k], ls.at[k], lr.at[k], peer(k))

    pair_sum = remote(lws.at[0], lws.at[1], ps, pr, partner)

    ag[0, core] = fields.astype(jnp.bfloat16)
    forward(0).start()

    def start_spread(k, c):
        spread(k).start()
        return c

    lax.fori_loop(1, chips, start_spread, 0)
    row = jnp.sum(fields * capped - 0.5 * capped * capped, axis=0, keepdims=True)
    lw[0] = jnp.broadcast_to(row, lw.shape[1:])

    def start_tell(k, c):
        tell(k).start()
        return c

    lax.fori_loop(1, chips, start_tell, 0)

    per_stage = chips // STAGES
    deep = total // STAGES
    own_stage = lax.div(chip, per_stage)
    cols = pot.shape[1]
    width = min(512, cols // 2)
    halves = cols // 2 // width

    def pull(s):
        def one(k, c):
            spread(k).wait_recv()
            forward(k).start()
            return c
        lax.fori_loop(max(1, s * per_stage), (s + 1) * per_stage, one, 0)

    def settle(s):
        def one(k, c):
            forward_in(k).wait_recv()
            return c
        lax.fori_loop(s * per_stage, (s + 1) * per_stage, one, 0)

    pull(0)
    settle(0)
    for s in range(STAGES):
        plane = flip(own_stage, s, 2)
        blocks = []
        for m in range(per_stage):
            k = flip(plane * per_stage + m, chip, bits)
            for c in range(2):
                block = ag[k, c]
                for j in range(pack):
                    blocks.append(block[:, j * walkers:(j + 1) * walkers])
        lhs[...] = jnp.concatenate(blocks, axis=0).T
        rows = pl.ds(pl.multiple_of(plane * deep, deep), deep)

        def column(t, c, s=s, rows=rows):
            at = pl.ds(pl.multiple_of(t * width, width), width)
            value = jnp.dot(lhs[...], fac[rows, at], preferred_element_type=jnp.float32)
            pot[:, at] = value if s == 0 else pot[:, at] + value
            return c

        lax.fori_loop(0, halves, column, 0)
        if s + 1 < STAGES:
            pull(s + 1)
        if s == STAGES - 2:
            def add(k, acc):
                tell(k).wait_recv()
                return acc + lw[k]
            lws[0] = lax.fori_loop(1, chips, add, lw[0])
            pair_sum.start()
        lax.fori_loop(halves, 2 * halves, column, 0)
        if s + 1 < STAGES:
            settle(s + 1)

    pair_sum.wait()
    packed = lws[0, 0:1, :] + lws[1, 0:1, :]
    row = packed[:, 0:walkers]
    for j in range(1, pack):
        row = row + packed[:, j * walkers:(j + 1) * walkers]
    per = walkers // n
    lane = lax.broadcasted_iota(jnp.int32, (1, walkers), 1)
    spot = lax.broadcasted_iota(jnp.int32, (1, per), 1)
    mine = jnp.zeros((1, per), jnp.float32)
    for j in range(per):
        one = jnp.sum(jnp.where(lane == me * per + j, row, 0.0), axis=1, keepdims=True)
        mine = jnp.where(spot == j, one, mine)
    logw[...] = (mine / math.sqrt(total)).reshape(per)

    d2d(0).wait_send()
    forward(0).wait_send()

    def drain(k, c):
        d2d(k).wait_send()
        scatter(k).wait_send()
        spread(k).wait_send()
        forward(k).wait_send()
        tell(k).wait_send()
        return c

    lax.fori_loop(1, chips, drain, 0)


def solution(mesh):
    n = mesh.shape["chol"]

    def per_device(green, factors, noise):
        walkers, cols = green.shape
        total = factors.shape[0]
        chips = n // 2
        pack = max(1, 128 // walkers)
        half, lanes = total // n // pack, walkers * pack
        vmem = pl.BlockSpec(memory_space=pltpu.VMEM)
        dma = pltpu.SemaphoreType.DMA
        block = pltpu.VMEM((chips, half, lanes), jnp.float32)
        pot, logw = pl.pallas_call(
            functools.partial(kernel, n, pack),
            out_shape=(jax.ShapeDtypeStruct((walkers, cols), jnp.float32),
                       jax.ShapeDtypeStruct((walkers // n,), jnp.float32)),
            in_specs=[vmem, pl.BlockSpec(memory_space=pl.ANY), vmem],
            out_specs=(vmem, vmem),
            scratch_shapes=[
                pltpu.VMEM(factors.shape, jnp.bfloat16),
                block, block, block, block,
                pltpu.VMEM((chips, 2, half, lanes), jnp.bfloat16),
                pltpu.VMEM((half, lanes), jnp.float32),
                pltpu.VMEM((walkers, total // STAGES), jnp.bfloat16),
                pltpu.VMEM((chips, 8, lanes), jnp.float32),
                pltpu.VMEM((2, 8, lanes), jnp.float32),
            ] + [dma((chips,))] * 11 + [dma, dma],
            compiler_params=pltpu.CompilerParams(
                collective_id=0, has_side_effects=True, vmem_limit_bytes=67043328),
        )(green, factors, noise)
        return pot, logw

    return jax.shard_map(
        per_device,
        mesh=mesh,
        in_specs=(P("groups", "chol"), P(None, "chol"), P("groups", "chol")),
        out_specs=(P("groups", "chol"), P(("groups", "chol"))),
        check_vma=False,
    )
```
